32 devices in a mesh: seq: 8 (over y, x, core), head: 4 (over z).
Axes of the slice: x: 2, y: 2, z: 4, core: 2. Of those that a mesh axis runs over, the one named last changes fastest.
Arguments:
- queries: bfloat16 [8, 32, 128], P('seq', 'head'), may hold values from -40 to 40
- key_pool: bfloat16 [288, 16, 128, 128], P('seq', 'head'), may hold values from -6 to 6
- value_pool: bfloat16 [288, 16, 128, 128], P('seq', 'head'), may hold values from -6 to 6
- lengths: int32 [8], replicated, may hold values from 2 to 16384, as said below
- block_table: int32 [8, 33], replicated, may hold values from -1 to 287, as said below
- out_weight: bfloat16 [4096, 4608], P('head'), may hold values from -0.09375 to 0.09375
Outputs:
- projected: bfloat16 [8, 4608], replicated
The draws below stay inside these ranges and needn't reach their ends.
Inputs may be any that keep to these rules, and one draw needn't show every extreme that they name: `lengths`: at least 2; some request has exactly 16384. `block_table`: for request b the first (L - 1) // 128 - max(L - 4096, 0) // 128 + 1 entries hold slots; the rest are -1. No slot appears twice in the table.
All inputs are finite; a program needn't handle non-finite values.
Results may differ from the reference program's by a relative error of at most 0.017.
Values may be sent and summed in bfloat16 or wider, within the bound.
A program may use at most 64 MiB of HBM per device.

```python
import jax
import jax.numpy as jnp
from jax import lax

D = 4608
HEADS = 32
KV_HEADS = 16
HD = 128
WINDOW = 4096
BLOCK = 128
MAXLEN = 16384
NBLK = 33
SLOTS = 288
BATCH = 8


def common_layout(key):
    base = jax.random.fold_in(key, 101)
    key_one, key_two, key_three = jax.random.split(base, 3)
    lengths = jax.random.randint(key_one, (BATCH,), 2, MAXLEN + 1).astype(jnp.int32)
    longest = jax.random.randint(key_three, (), 0, BATCH)
    lengths = lengths.at[longest].set(MAXLEN)
    window_start = jnp.maximum(lengths - WINDOW, 0)
    first_block = window_start // BLOCK
    last_block = (lengths - 1) // BLOCK
    count = last_block - first_block + 1
    live = jnp.arange(NBLK, dtype=jnp.int32)[None, :] < count[:, None]
    flat_live = live.reshape(-1)
    order = jnp.cumsum(flat_live.astype(jnp.int32)) - 1
    shuffled = jax.random.permutation(key_two, SLOTS).astype(jnp.int32)
    table = jnp.where(flat_live, shuffled[jnp.clip(order, 0, SLOTS - 1)], -1)
    return (lengths, table.reshape(BATCH, NBLK).astype(jnp.int32), first_block)


def aligned_signs(key):
    coins = jax.random.bernoulli(jax.random.fold_in(key, 202), 0.5, (4, KV_HEADS, HD))
    return jnp.where(coins, 1.0, -1.0).astype(jnp.float32)


def query_strengths():
    return jnp.array([6.0, 10.0, 15.0, 20.0], jnp.float32)


def draw_lengths(key, part):
    return common_layout(key)[0]


def draw_block_table(key, part):
    return common_layout(key)[1]


def draw_queries(key, part):
    fresh = jax.random.fold_in(key, 303)
    drawn = jnp.clip(jax.random.normal(fresh, (BATCH, HEADS, HD)), -6.0, 6.0)
    signs = jnp.repeat(aligned_signs(key), HEADS // KV_HEADS, axis=1)
    drawn = drawn.at[0:4].set(signs * query_strengths()[:, None, None])
    return drawn.astype(jnp.bfloat16)


def draw_key_pool(key, part):
    fresh = jax.random.fold_in(key, 404)
    drawn = jnp.clip(jax.random.normal(fresh, (SLOTS, KV_HEADS, BLOCK, HD)), -6.0, 6.0)
    lengths, table, first_block = common_layout(key)
    signs = aligned_signs(key) * 5.5
    strengths = query_strengths()
    for request in range(4):
        length = lengths[request]
        slot_last = table[request, (length - 1) // BLOCK - first_block[request]]
        slot_prior = table[request, (length - 2) // BLOCK - first_block[request]]
        top_key = signs[request]
        lowered = jnp.abs(top_key[:, 0]) - 24.0 / strengths[request]
        prior_key = top_key.at[:, 0].set(jnp.sign(top_key[:, 0]) * lowered)
        drawn = drawn.at[slot_last, :, (length - 1) % BLOCK, :].set(top_key)
        drawn = drawn.at[slot_prior, :, (length - 2) % BLOCK, :].set(prior_key)
    return drawn.astype(jnp.bfloat16)


def levels(rng, dims, shards, low, high):
    gain, own = 1.0, jax.random.fold_in(rng, 6)
    for position, parts in shards:
        draws = jnp.exp(jax.random.uniform(jax.random.fold_in(own, position), (parts,), jnp.float32, low / len(shards), high / len(shards)))
        gain = gain * jnp.repeat(draws, dims[position] // parts).reshape([-1 if axis == position else 1 for axis in range(len(dims))])
    return gain


def gaussian(own_key, extent, width, limit, pieces=(), kind=jnp.bfloat16):
    level = levels(own_key, extent, pieces, -0.22, 0.18) if pieces else 1.0
    values = jax.random.normal(own_key, extent, jnp.float32) * width * level
    return jnp.minimum(jnp.maximum(values, -limit), limit).astype(kind)


def setup_inputs(seed: int = 0) -> dict:
    arg_keys = jax.random.split(jax.random.key(seed), 7)
    queries = draw_queries(jax.random.fold_in(arg_keys[6], 71), 0)
    key_pool = draw_key_pool(jax.random.fold_in(arg_keys[6], 71), 0)
    value_pool = gaussian(arg_keys[2], (SLOTS, KV_HEADS, BLOCK, HD), 1.0, 6.0, ((0, 8), (1, 4)))
    lengths = draw_lengths(jax.random.fold_in(arg_keys[6], 71), 0)
    block_table = draw_block_table(jax.random.fold_in(arg_keys[6], 71), 0)
    out_weight = gaussian(arg_keys[5], (HEADS * HD, D), (HEADS * HD) ** -0.5, 0.09375, ((0, 4),))
    return {"queries": queries, "key_pool": key_pool, "value_pool": value_pool, "lengths": lengths, "block_table": block_table, "out_weight": out_weight}


lowest_score = -1e30
score_scale = 1.0 / 12.0


def one_request(request, key_pool, value_pool):
    length, table_row, query = request
    window_start = jnp.maximum(length - WINDOW, 0)
    first_block = window_start // BLOCK
    safe_rows = jnp.maximum(table_row, 0).astype(jnp.int32)
    keys = key_pool[safe_rows].astype(jnp.float32)
    values = value_pool[safe_rows].astype(jnp.float32)
    offset = jnp.arange(NBLK, dtype=jnp.int32)
    inside = jnp.arange(BLOCK, dtype=jnp.int32)
    positions = (first_block + offset)[:, None] * BLOCK + inside[None, :]
    in_window = (table_row >= 0)[:, None] & (positions >= window_start) & (positions < length)
    grouped = query.astype(jnp.float32).reshape(KV_HEADS, HEADS // KV_HEADS, HD)
    scores = jnp.einsum('kgd,jktd->kgjt', grouped, keys).reshape(HEADS, NBLK, BLOCK) * score_scale
    masked = jnp.where(in_window[None], scores, lowest_score)
    largest = jnp.max(masked, axis=(1, 2))
    weights = jnp.where(in_window[None], jnp.exp(scores - largest[:, None, None]), 0.0)
    total = jnp.sum(weights, axis=(1, 2))
    rounded = weights.astype(jnp.bfloat16).astype(jnp.float32)
    rounded = rounded.reshape(KV_HEADS, HEADS // KV_HEADS, NBLK, BLOCK)
    summed = jnp.einsum('kgjt,jktd->kgd', rounded, values).reshape(HEADS, HD)
    return (summed / total[:, None]).astype(jnp.bfloat16)


def reference(queries, key_pool, value_pool, lengths, block_table, out_weight):
    attention = lax.map(lambda request: one_request(request, key_pool, value_pool), (lengths, block_table, queries))
    flat = attention.reshape(BATCH, HEADS * HD)
    return jnp.dot(flat, out_weight, preferred_element_type=jnp.float32).astype(jnp.bfloat16)
```

```python
import functools

import jax
import jax.numpy as jnp
from jax import lax
from jax.experimental import pallas as pl
from jax.experimental.pallas import tpu as pltpu
from jax.sharding import PartitionSpec as P

WINDOW = 4096

lowest_score = -1e30
lowest_largest = -1e29
score_scale = 1.0 / 12.0
LANES = 128
F32 = jnp.float32
BF16 = jnp.bfloat16
MESH = pl.DeviceIdType.MESH


def column_tiles(width, parts):
    tiles = width // LANES
    starts = [tiles * i // parts for i in range(parts)]
    ends = starts[1:] + [tiles]
    span = max(e - s for s, e in zip(starts, ends))
    return tiles, starts, ends, span


def peer_index(index, step, size):
    if size & (size - 1):
        return lax.rem(index + step, size)
    peer, bit = 0, 1
    while bit < size:
        own = lax.rem(lax.div(index, bit), 2)
        peer = peer + bit * ((1 - own) if step & bit else own)
        bit *= 2
    return peer


def kernel(
    n, nz,
    q_hbm, k_hbm, v_hbm, len_hbm, tab_hbm, w_hbm, out_ref,
    kbuf, vbuf, wbuf, qall, qf, tabv, lens, bias, scores, probs,
    mlbuf, obuf, wts, zbuf, fbuf,
    in_sem, k_sem, v_sem, q_send, q_recv, ml_send, ml_recv,
    o_send, o_recv, z_send, z_recv, f_send, f_recv, seq_ready, head_ready,
):
    me = lax.axis_index("seq")
    mz = lax.axis_index("head")
    slot_count, kv_count, block_len, head_width = k_hbm.shape
    batch, entries = tab_hbm.shape
    own_batch, head_count = q_hbm.shape[0], q_hbm.shape[1]
    group = head_count // kv_count
    tiles, starts, ends, span = column_tiles(w_hbm.shape[1], n)
    total_columns = slot_count * block_len
    seq_peer = [peer_index(me, j, n) for j in range(n)]
    head_peer = [peer_index(mz, j, nz) for j in range(nz)]

    barrier = pltpu.get_barrier_semaphore()
    greets_seq = lax.rem(me, 2) == 1
    partner = seq_peer[1]
    others = [lax.rem(mz + j, nz) for j in range(1, nz)]
    chip = me - lax.rem(me, 2)
    for j in reversed(range(1, n)):
        peer = seq_peer[j]

        @pl.when(lax.rem(peer, 2) == 1)
        def _():
            pl.semaphore_signal(barrier, inc=1, device_id={"seq": peer}, device_id_type=MESH)

    for z in others:
        pl.semaphore_signal(
            barrier, inc=1, device_id={"seq": chip, "head": z}, device_id_type=MESH
        )

    own_rows = pl.ds(me * own_batch, own_batch)
    q_in = pltpu.make_async_copy(q_hbm, qall.at[own_rows], in_sem.at[0])
    tab_in = pltpu.make_async_copy(tab_hbm, tabv, in_sem.at[1])
    len_in = pltpu.make_async_copy(len_hbm, lens, in_sem.at[2])
    first_column = pl.multiple_of((tiles * me // n) * LANES, LANES)
    w_in = pltpu.make_async_copy(
        w_hbm.at[:, pl.ds(first_column, span * LANES)], wbuf, in_sem.at[3]
    )
    k_in = [pltpu.make_async_copy(k_hbm.at[:, k], kbuf.at[k], k_sem.at[k]) for k in range(kv_count)]
    v_in = [pltpu.make_async_copy(v_hbm.at[:, k], vbuf.at[k], v_sem.at[k]) for k in range(kv_count)]
    for copy in [q_in, tab_in, len_in]:
        copy.start()
    for copy in [q_in, tab_in, len_in]:
        copy.wait()
    for copy in k_in + v_in + [w_in]:
        copy.start()

    def to_seq(ref, send, recv):
        copies = []
        for j in reversed(range(1, n)):
            copies.append(
                pltpu.make_async_remote_copy(
                    src_ref=ref, dst_ref=ref, send_sem=send(j), recv_sem=recv(j),
                    device_id={"seq": seq_peer[j]}, device_id_type=MESH,
                )
            )
        for copy in copies:
            copy.start()
        return copies

    @pl.when(greets_seq)
    def _():
        pl.semaphore_wait(barrier, n - 1)
        pl.semaphore_signal(seq_ready, inc=1, device_id={"seq": partner}, device_id_type=MESH)

    @pl.when(jnp.logical_not(greets_seq))
    def _():
        pl.semaphore_wait(seq_ready, 1)

    q_copies = to_seq(qall.at[own_rows], lambda j: q_send.at[j], lambda j: q_recv.at[j])

    row = lax.broadcasted_iota(jnp.int32, (batch, LANES), 0)
    lane = lax.broadcasted_iota(jnp.int32, (batch, LANES), 1)
    length = jnp.zeros((batch, LANES), jnp.int32)
    for b in range(batch):
        length = jnp.where(row == b, lens[b], length)
    window_start = jnp.maximum(length - WINDOW, 0)
    first_block = lax.div(window_start, block_len)
    table = tabv[...]
    slot_lane = lane + me * slot_count
    rank = jnp.full((batch, LANES), -1, jnp.int32)
    for j in range(entries):
        rank = jnp.where(table[:, j : j + 1] == slot_lane, j, rank)
    base = (first_block + rank) * block_len
    low = jnp.where(rank >= 0, window_start - base, block_len)
    high = jnp.where(rank >= 0, length - base, 0)
    for p in range(slot_count):
        live = (lane >= low[:, p : p + 1]) & (lane < high[:, p : p + 1])
        bias[:, p * block_len : (p + 1) * block_len] = jnp.where(live, 0.0, lowest_score)

    for copy in k_in + v_in + [w_in]:
        copy.wait()
    for copy in q_copies:
        copy.wait_recv()
    for b in range(batch):
        qf[b * head_count : (b + 1) * head_count, :] = qall[b].astype(F32)

    chunk = 4 if slot_count % 4 == 0 else 1
    width = chunk * block_len
    chunks = slot_count // chunk
    rows = group * batch

    def lane_tiles(x, op):
        out = x[:, :LANES]
        for c in range(1, x.shape[1] // LANES):
            out = op(out, x[:, c * LANES : (c + 1) * LANES])
        return out

    largest, totals = [], []

    def score(k):
        grouped = jnp.concatenate(
            [qf[pl.ds(k * group + g, batch, stride=head_count), :] for g in range(group)], axis=0
        ).astype(BF16)
        top = jnp.full((rows, LANES), lowest_largest, F32)
        for c in range(chunks):
            keys = kbuf[k, c * chunk : (c + 1) * chunk].reshape(width, head_width)
            s = lax.dot_general(
                grouped, keys, (((1,), (1,)), ((), ())), preferred_element_type=F32
            )
            mask = bias[:, c * width : (c + 1) * width]
            s = s * score_scale + jnp.concatenate([mask] * group, axis=0)
            scores[k, :, c * width : (c + 1) * width] = s
            top = jnp.maximum(top, lane_tiles(s, jnp.maximum))
        largest.append(jnp.max(top, axis=1, keepdims=True))

    def soften(k):
        total = jnp.zeros((rows, LANES), F32)
        for c in range(chunks):
            weight = jnp.exp(scores[k, :, c * width : (c + 1) * width] - largest[k])
            total = total + lane_tiles(weight, jnp.add)
            probs[k, :, c * width : (c + 1) * width] = weight.astype(BF16)
        totals.append(jnp.sum(total, axis=1, keepdims=True))

    def share_totals():
        packed_largest = jnp.zeros((batch, LANES), F32)
        packed_total = jnp.ones((batch, LANES), F32)
        for k in range(kv_count):
            for g in range(group):
                h = k * group + g
                part = slice(g * batch, (g + 1) * batch)
                packed_largest = jnp.where(lane == h, largest[k][part], packed_largest)
                packed_total = jnp.where(lane == h, totals[k][part], packed_total)
        mlbuf[me, 0] = packed_largest
        mlbuf[me, 1] = packed_total
        return to_seq(mlbuf.at[me], lambda j: ml_send.at[j], lambda j: ml_recv.at[j])

    def share_sums(k):
        values = vbuf[k].reshape(total_columns, head_width)
        summed = jnp.dot(probs[k], values, preferred_element_type=F32)
        obuf[me, k] = summed.astype(BF16)
        return to_seq(obuf.at[me, k], lambda j: o_send.at[j, k], lambda j: o_recv.at[j, k])

    o_copies = []
    for k in range(kv_count):
        score(k)
    for k in range(kv_count):
        soften(k)
    ml_copies = share_totals()
    for k in range(kv_count):
        o_copies.append(share_sums(k))

    for copy in ml_copies:
        copy.wait_recv()
    whole_largest = mlbuf[0, 0]
    for i in range(1, n):
        whole_largest = jnp.maximum(whole_largest, mlbuf[i, 0])
    whole_total = jnp.zeros((batch, LANES), F32)
    factors = []
    for i in range(n):
        factors.append(jnp.exp(mlbuf[i, 0] - whole_largest))
        whole_total = whole_total + factors[i] * mlbuf[i, 1]
    inverse = 1.0 / whole_total
    for i in range(n):
        factor = factors[i] * inverse
        for h in range(head_count):
            wts[i, h] = jnp.broadcast_to(factor[:, h : h + 1], (batch, LANES))

    partial_sum = jnp.zeros((batch, span * LANES), F32)
    for k in range(kv_count):
        for copy in o_copies[k]:
            copy.wait_recv()
        parts = [jnp.zeros((batch, head_width), F32) for _ in range(group)]
        for i in range(n):
            arrived = obuf[i, k].astype(F32)
            for g in range(group):
                parts[g] = parts[g] + wts[i, k * group + g] * arrived[g * batch : (g + 1) * batch]
        attention = jnp.concatenate(parts, axis=1).astype(BF16)
        depth = group * head_width
        partial_sum = partial_sum + jnp.dot(
            attention, wbuf[k * depth : (k + 1) * depth, :], preferred_element_type=F32
        )

    @pl.when(jnp.logical_not(greets_seq))
    def _():
        pl.semaphore_wait(barrier, 2 * (nz - 1))
        pl.semaphore_signal(head_ready, inc=1, device_id={"seq": partner}, device_id_type=MESH)

    @pl.when(greets_seq)
    def _():
        pl.semaphore_wait(head_ready, 1)

    zbuf[mz] = partial_sum.astype(BF16)
    z_copies = []
    for j in reversed(range(1, nz)):
        z_copies.append(
            pltpu.make_async_remote_copy(
                src_ref=zbuf.at[mz], dst_ref=zbuf.at[mz],
                send_sem=z_send.at[j], recv_sem=z_recv.at[j],
                device_id={"head": head_peer[j]}, device_id_type=MESH,
            )
        )
    for copy in z_copies:
        copy.start()
    for copy in z_copies:
        copy.wait_recv()
    finished = zbuf[0].astype(F32)
    for i in range(1, nz):
        finished = finished + zbuf[i].astype(F32)
    fbuf[me] = finished.astype(BF16)
    f_copies = to_seq(fbuf.at[me], lambda j: f_send.at[j], lambda j: f_recv.at[j])
    for copy in f_copies:
        copy.wait_recv()
    for i in range(n):
        if ends[i] > starts[i]:
            out_ref[:, starts[i] * LANES : ends[i] * LANES] = fbuf[
                i, :, : (ends[i] - starts[i]) * LANES
            ]
    for copy in q_copies + ml_copies + z_copies + f_copies:
        copy.wait_send()
    for copies in o_copies:
        for copy in copies:
            copy.wait_send()


def local(n, nz, queries, key_pool, value_pool, lengths, block_table, out_weight):
    slot_count, kv_count, block_len, head_width = key_pool.shape
    batch, entries = block_table.shape
    head_count = queries.shape[1]
    rows = head_count // kv_count * batch
    columns = slot_count * block_len
    depth, out_width = out_weight.shape
    _, _, _, span = column_tiles(out_width, n)
    dma = pltpu.SemaphoreType.DMA
    hbm = pl.BlockSpec(memory_space=pl.ANY)
    return pl.pallas_call(
        functools.partial(kernel, n, nz),
        out_shape=pltpu.VMEM((batch, out_width), BF16),
        in_specs=[hbm] * 6,
        out_specs=pl.BlockSpec(memory_space=pltpu.VMEM),
        scratch_shapes=[
            pltpu.VMEM((kv_count, slot_count, block_len, head_width), BF16),
            pltpu.VMEM((kv_count, slot_count, block_len, head_width), BF16),
            pltpu.VMEM((depth, span * LANES), BF16),
            pltpu.VMEM((batch, head_count, head_width), BF16),
            pltpu.VMEM((batch * head_count, head_width), F32),
            pltpu.VMEM((batch, entries), jnp.int32),
            pltpu.SMEM((batch,), jnp.int32),
            pltpu.VMEM((batch, columns), F32),
            pltpu.VMEM((kv_count, rows, columns), F32),
            pltpu.VMEM((kv_count, rows, columns), BF16),
            pltpu.VMEM((n, 2, batch, LANES), F32),
            pltpu.VMEM((n, kv_count, rows, head_width), BF16),
            pltpu.VMEM((n, head_count, batch, LANES), F32),
            pltpu.VMEM((nz, batch, span * LANES), BF16),
            pltpu.VMEM((n, batch, span * LANES), BF16),
            dma((4,)), dma((kv_count,)), dma((kv_count,)),
            dma((n,)), dma((n,)), dma((n,)), dma((n,)),
            dma((n, kv_count)), dma((n, kv_count)),
            dma((nz,)), dma((nz,)), dma((n,)), dma((n,)),
            pltpu.SemaphoreType.REGULAR, pltpu.SemaphoreType.REGULAR,
        ],
        compiler_params=pltpu.CompilerParams(
            collective_id=0, has_side_effects=True, vmem_limit_bytes=56 * 1024 * 1024
        ),
    )(queries, key_pool, value_pool, lengths, block_table, out_weight)


def solution(mesh):
    return jax.shard_map(
        functools.partial(local, mesh.shape["seq"], mesh.shape["head"]),
        mesh=mesh,
        in_specs=(
            P("seq", "head", None),
            P("seq", "head", None, None),
            P("seq", "head", None, None),
            P(),
            P(),
            P("head", None),
        ),
        out_specs=P(),
        check_vma=False,
    )
```

```python
import functools

import jax
import jax.numpy as jnp
from jax import lax
from jax.experimental import pallas as pl
from jax.experimental.pallas import tpu as pltpu
from jax.sharding import PartitionSpec as P

WINDOW = 4096

lowest_score = -1e30
lowest_largest = -1e29
score_scale = 1.0 / 12.0
LANES = 128
F32 = jnp.float32
BF16 = jnp.bfloat16
MESH = pl.DeviceIdType.MESH


def column_tiles(width, parts):
    tiles = width // LANES
    starts = [tiles * i // parts for i in range(parts)]
    ends = starts[1:] + [tiles]
    span = max(e - s for s, e in zip(starts, ends))
    return tiles, starts, ends, span


def batch_split(n, batch):
    return 2 if n % 2 == 0 and batch % 2 == 0 else 1


def peer_index(index, step, size):
    if size & (size - 1):
        return lax.rem(index + step, size)
    peer, bit = 0, 1
    while bit < size:
        own = lax.rem(lax.div(index, bit), 2)
        peer = peer + bit * ((1 - own) if step & bit else own)
        bit *= 2
    return peer


def kernel(
    n, nz,
    q_hbm, k_hbm, v_hbm, len_hbm, tab_hbm, w_hbm, out_ref,
    kbuf, vbuf, wbuf, kflip, qall, qf, tabv, lens, bias, scores, probs,
    mlown, mlbuf, oown, obuf, wts, zbuf, fbuf,
    in_sem, k_sem, q_sem, ml_sem, o_send, o_recv, z_sem, f_sem,
):
    me = lax.axis_index("seq")
    mz = lax.axis_index("head")
    slot_count, kv_count, block_len, head_width = k_hbm.shape
    batch, entries = tab_hbm.shape
    own_batch, head_count = q_hbm.shape[0], q_hbm.shape[1]
    group = head_count // kv_count
    split = batch_split(n, batch)
    parts, share = n // split, batch // split
    rows = group * share
    tiles, starts, ends, span = column_tiles(w_hbm.shape[1], parts)
    total_columns = slot_count * block_len
    seq_peer = [peer_index(me, j, n) for j in range(n)]
    head_peer = [peer_index(mz, j, nz) for j in range(nz)]

    barrier = pltpu.get_barrier_semaphore()
    for j in reversed(range(1, n)):
        pl.semaphore_signal(barrier, inc=1, device_id={"seq": seq_peer[j]}, device_id_type=MESH)
    for j in reversed(range(1, nz)):
        pl.semaphore_signal(barrier, inc=1, device_id={"head": head_peer[j]}, device_id_type=MESH)

    own_rows = pl.ds(me * own_batch, own_batch)
    q_in = pltpu.make_async_copy(q_hbm, qall.at[own_rows], in_sem.at[0])
    tab_in = pltpu.make_async_copy(tab_hbm, tabv, in_sem.at[1])
    len_in = pltpu.make_async_copy(len_hbm, lens, in_sem.at[2])
    first_column = pl.multiple_of((tiles * lax.div(me, split) // parts) * LANES, LANES)
    w_in = pltpu.make_async_copy(
        w_hbm.at[:, pl.ds(first_column, span * LANES)], wbuf, in_sem.at[3]
    )
    k_in = [pltpu.make_async_copy(k_hbm.at[:, k], kbuf.at[k], k_sem.at[k]) for k in range(kv_count)]
    v_in = [pltpu.make_async_copy(v_hbm.at[:, k], vbuf.at[k], in_sem.at[4]) for k in range(kv_count)]
    for copy in [q_in, tab_in, len_in]:
        copy.start()
    for copy in [q_in, tab_in, len_in]:
        copy.wait()
    for copy in k_in + v_in + [w_in]:
        copy.start()

    def to_seq(source, target, send, recv):
        copies = []
        for j in reversed(range(1, n)):
            copies.append(
                pltpu.make_async_remote_copy(
                    src_ref=source(seq_peer[j]), dst_ref=target, send_sem=send, recv_sem=recv,
                    device_id={"seq": seq_peer[j]}, device_id_type=MESH,
                )
            )
        for copy in copies:
            copy.start()

    def wait_all(ref, sem):
        pltpu.make_async_copy(ref, ref, sem).wait()

    pl.semaphore_wait(barrier, n - 1 + nz - 1)
    to_seq(lambda peer: qall.at[own_rows], qall.at[own_rows], q_sem.at[0], q_sem.at[1])

    def by_rows(x):
        return jnp.concatenate(
            [x[s * share : (s + 1) * share] for s in range(split) for _ in range(group)], axis=0
        )

    all_rows = split * rows
    row = lax.broadcasted_iota(jnp.int32, (batch, LANES), 0)
    lane = lax.broadcasted_iota(jnp.int32, (batch, LANES), 1)
    length = jnp.zeros((batch, LANES), jnp.int32)
    for b in range(batch):
        length = jnp.where(row == b, lens[b], length)
    window_start = jnp.maximum(length - WINDOW, 0)
    first_block = lax.div(window_start, block_len)
    table = tabv[...]
    slot_lane = lane + me * slot_count
    rank = jnp.full((batch, LANES), -1, jnp.int32)
    for j in range(entries):
        rank = jnp.where(table[:, j : j + 1] == slot_lane, j, rank)
    base = (first_block + rank) * block_len
    low = by_rows(jnp.where(rank >= 0, window_start - base, block_len))
    high = by_rows(jnp.where(rank >= 0, length - base, 0))
    lane = lax.broadcasted_iota(jnp.int32, (all_rows, LANES), 1)
    for p in range(slot_count):
        live = (lane >= low[:, p : p + 1]) & (lane < high[:, p : p + 1])
        bias[:, p * block_len : (p + 1) * block_len] = jnp.where(live, 0.0, lowest_score)

    for k in range(kv_count):
        k_in[k].wait()
        for p in range(slot_count):
            kflip[k, :, p * block_len : (p + 1) * block_len] = kbuf[k, p].T

    wait_all(vbuf, in_sem.at[4])
    wait_all(qall.at[pl.ds(0, (n - 1) * own_batch)], q_sem.at[1])
    for b in range(batch):
        qf[b * head_count : (b + 1) * head_count, :] = qall[b].astype(F32)

    chunk = 4 if slot_count % 4 == 0 else 1
    width = chunk * block_len
    chunks = slot_count // chunk

    def lane_tiles(x, op):
        out = x[:, :LANES]
        for c in range(1, x.shape[1] // LANES):
            out = op(out, x[:, c * LANES : (c + 1) * LANES])
        return out

    largest, totals = [], []

    def score(k):
        grouped = jnp.concatenate(
            [
                qf[pl.ds(s * share * head_count + k * group + g, share, stride=head_count), :]
                for s in range(split)
                for g in range(group)
            ],
            axis=0,
        ).astype(BF16)
        top = jnp.full((all_rows, LANES), lowest_largest, F32)
        for c in range(chunks):
            part = slice(c * width, (c + 1) * width)
            s = jnp.dot(grouped, kflip[k, :, part], preferred_element_type=F32)
            s = s * score_scale + bias[:, part]
            scores[k, :, part] = s
            top = jnp.maximum(top, lane_tiles(s, jnp.maximum))
        largest.append(jnp.max(top, axis=1, keepdims=True))

    def soften(k):
        total = jnp.zeros((all_rows, LANES), F32)
        for c in range(chunks):
            part = slice(c * width, (c + 1) * width)
            weight = jnp.exp(scores[k, :, part] - largest[k])
            total = total + lane_tiles(weight, jnp.add)
            probs[k, :, part] = weight.astype(BF16)
        totals.append(jnp.sum(total, axis=1, keepdims=True))

    own_share = lax.rem(me, split)

    def share_totals():
        packed = jnp.ones((all_rows, LANES), F32)
        for k in range(kv_count):
            packed = jnp.where(lane == k, largest[k], packed)
            packed = jnp.where(lane == kv_count + k, totals[k], packed)
        for s in range(split):
            mlown[s] = packed[s * rows : (s + 1) * rows]
        mlbuf[me] = mlown[own_share]
        to_seq(
            lambda peer: mlown.at[lax.rem(peer, split)], mlbuf.at[me], ml_sem.at[0], ml_sem.at[1]
        )

    def share_sums(k):
        values = vbuf[k].reshape(total_columns, head_width)
        summed = jnp.dot(probs[k], values, preferred_element_type=F32).astype(BF16)
        for s in range(split):
            oown[k, s] = summed[s * rows : (s + 1) * rows]
        obuf[k, me] = oown[k, own_share]
        to_seq(
            lambda peer: oown.at[k, lax.rem(peer, split)], obuf.at[k, me], o_send.at[0], o_recv.at[k]
        )

    for k in range(kv_count):
        score(k)
    for k in range(kv_count):
        soften(k)
    share_totals()
    for k in range(kv_count):
        share_sums(k)

    others = pl.ds(0, n - 1)
    wait_all(mlbuf.at[others], ml_sem.at[1])
    whole_largest = mlbuf[0]
    for i in range(1, n):
        whole_largest = jnp.maximum(whole_largest, mlbuf[i])
    whole_total = jnp.zeros((rows, LANES), F32)
    factors = []
    for i in range(n):
        factors.append(jnp.exp(jnp.minimum(mlbuf[i] - whole_largest, 0.0)))
        whole_total = whole_total + factors[i] * pltpu.roll(mlbuf[i], LANES - kv_count, 1)
    inverse = 1.0 / whole_total
    for i in range(n):
        factor = factors[i] * inverse
        for k in range(kv_count):
            wts[i, k] = jnp.broadcast_to(factor[:, k : k + 1], (rows, head_width))

    w_in.wait()
    partial_sum = jnp.zeros((share, span * LANES), F32)
    depth = group * head_width
    for k in range(kv_count):
        wait_all(obuf.at[k, others], o_recv.at[k])
        part = jnp.zeros((rows, head_width), F32)
        for i in range(n):
            part = part + wts[i, k] * obuf[k, i].astype(F32)
        attention = jnp.concatenate(
            [part[g * share : (g + 1) * share] for g in range(group)], axis=1
        ).astype(BF16)
        partial_sum = partial_sum + jnp.dot(
            attention, wbuf[k * depth : (k + 1) * depth, :], preferred_element_type=F32
        )

    zbuf[mz] = partial_sum.astype(BF16)
    for j in reversed(range(1, nz)):
        pltpu.make_async_remote_copy(
            src_ref=zbuf.at[mz], dst_ref=zbuf.at[mz], send_sem=z_sem.at[0], recv_sem=z_sem.at[1],
            device_id={"head": head_peer[j]}, device_id_type=MESH,
        ).start()
    wait_all(zbuf.at[pl.ds(0, nz - 1)], z_sem.at[1])
    finished = zbuf[0].astype(F32)
    for z in range(1, nz):
        finished = finished + zbuf[z].astype(F32)
    fbuf[me] = finished.astype(BF16)
    to_seq(lambda peer: fbuf.at[me], fbuf.at[me], f_sem.at[0], f_sem.at[1])
    wait_all(fbuf.at[others], f_sem.at[1])
    for c in range(parts):
        if ends[c] > starts[c]:
            filled = (ends[c] - starts[c]) * LANES
            out_ref[:, starts[c] * LANES : ends[c] * LANES] = jnp.concatenate(
                [fbuf[c * split + s, :, :filled] for s in range(split)], axis=0
            )
    wait_all(qall.at[pl.ds(0, (n - 1) * own_batch)], q_sem.at[0])
    wait_all(mlbuf.at[others], ml_sem.at[0])
    wait_all(obuf.at[:, others], o_send.at[0])
    wait_all(zbuf.at[pl.ds(0, nz - 1)], z_sem.at[0])
    wait_all(fbuf.at[others], f_sem.at[0])


def local(n, nz, queries, key_pool, value_pool, lengths, block_table, out_weight):
    slot_count, kv_count, block_len, head_width = key_pool.shape
    batch, entries = block_table.shape
    head_count = queries.shape[1]
    split = batch_split(n, batch)
    share = batch // split
    rows = head_count // kv_count * share
    columns = slot_count * block_len
    depth, out_width = out_weight.shape
    _, _, _, span = column_tiles(out_width, n // split)
    dma = pltpu.SemaphoreType.DMA
    hbm = pl.BlockSpec(memory_space=pl.ANY)
    return pl.pallas_call(
        functools.partial(kernel, n, nz),
        out_shape=pltpu.VMEM((batch, out_width), BF16),
        in_specs=[hbm] * 6,
        out_specs=pl.BlockSpec(memory_space=pltpu.VMEM),
        scratch_shapes=[
            pltpu.VMEM((kv_count, slot_count, block_len, head_width), BF16),
            pltpu.VMEM((kv_count, slot_count, block_len, head_width), BF16),
            pltpu.VMEM((depth, span * LANES), BF16),
            pltpu.VMEM((kv_count, head_width, columns), BF16),
            pltpu.VMEM((batch, head_count, head_width), BF16),
            pltpu.VMEM((batch * head_count, head_width), F32),
            pltpu.VMEM((batch, entries), jnp.int32),
            pltpu.SMEM((batch,), jnp.int32),
            pltpu.VMEM((split * rows, columns), F32),
            pltpu.VMEM((kv_count, split * rows, columns), F32),
            pltpu.VMEM((kv_count, split * rows, columns), BF16),
            pltpu.VMEM((split, rows, LANES), F32),
            pltpu.VMEM((n, rows, LANES), F32),
            pltpu.VMEM((kv_count, split, rows, head_width), BF16),
            pltpu.VMEM((kv_count, n, rows, head_width), BF16),
            pltpu.VMEM((n, kv_count, rows, head_width), F32),
            pltpu.VMEM((nz, share, span * LANES), BF16),
            pltpu.VMEM((n, share, span * LANES), BF16),
            dma((5,)), dma((kv_count,)), dma((2,)), dma((2,)),
            dma((1,)), dma((kv_count,)), dma((2,)), dma((2,)),
        ],
        compiler_params=pltpu.CompilerParams(
            collective_id=0, has_side_effects=True, vmem_limit_bytes=56 * 1024 * 1024
        ),
    )(queries, key_pool, value_pool, lengths, block_table, out_weight)


def solution(mesh):
    return jax.shard_map(
        functools.partial(local, mesh.shape["seq"], mesh.shape["head"]),
        mesh=mesh,
        in_specs=(
            P("seq", "head", None),
            P("seq", "head", None, None),
            P("seq", "head", None, None),
            P(),
            P(),
            P("head", None),
        ),
        out_specs=P(),
        check_vma=False,
    )
```

```python
import functools

import jax
import jax.numpy as jnp
from jax import lax
from jax.experimental import pallas as pl
from jax.experimental.pallas import tpu as pltpu
from jax.sharding import PartitionSpec as P

WINDOW = 4096

lowest_score = -1e30
lowest_largest = -1e29
score_scale = 1.0 / 12.0
LANES = 128
F32 = jnp.float32
BF16 = jnp.bfloat16
MESH = pl.DeviceIdType.MESH


def column_tiles(width, parts):
    tiles = width // LANES
    starts = [tiles * i // parts for i in range(parts)]
    ends = starts[1:] + [tiles]
    span = max(e - s for s, e in zip(starts, ends))
    return tiles, starts, ends, span


def cores_of(n):
    return 2 if n % 2 == 0 else 1


def peer_index(index, step, size):
    if size & (size - 1):
        return lax.rem(index + step, size)
    peer, bit = 0, 1
    while bit < size:
        own = lax.rem(lax.div(index, bit), 2)
        peer = peer + bit * ((1 - own) if step & bit else own)
        bit *= 2
    return peer


def kernel(
    n, nz,
    q_hbm, k_hbm, v_hbm, len_hbm, tab_hbm, w_hbm, out_ref,
    kbuf, vbuf, wbuf, kflip, qall, qf, tabv, lens, bias, scores, probs,
    mlbuf, obuf, wts, zbuf, fbuf,
    in_sem, k_sem, q_sem, ml_sem, o_send, o_recv, z_sem, f_sem,
):
    me = lax.axis_index("seq")
    mz = lax.axis_index("head")
    slot_count, kv_count, block_len, head_width = k_hbm.shape
    batch, entries = tab_hbm.shape
    own_batch, head_count = q_hbm.shape[0], q_hbm.shape[1]
    group = head_count // kv_count
    cores = cores_of(n)
    parts, part = n // cores, lax.div(me, cores)
    rows = group * batch
    tiles, starts, ends, span = column_tiles(w_hbm.shape[1], parts)

    def owns(index):
        return lax.rem(index, cores) == cores - 1

    total_columns = slot_count * block_len
    seq_peer = [peer_index(me, j, n) for j in range(n)]
    head_peer = [peer_index(mz, j, nz) for j in range(nz)]

    barrier = pltpu.get_barrier_semaphore()
    for j in reversed(range(1, n)):
        pl.semaphore_signal(barrier, inc=1, device_id={"seq": seq_peer[j]}, device_id_type=MESH)

    @pl.when(owns(me))
    def _():
        for j in reversed(range(1, nz)):
            pl.semaphore_signal(
                barrier, inc=1, device_id={"head": head_peer[j]}, device_id_type=MESH
            )

    own_rows = pl.ds(me * own_batch, own_batch)
    q_in = pltpu.make_async_copy(q_hbm, qall.at[own_rows], in_sem.at[0])
    tab_in = pltpu.make_async_copy(tab_hbm, tabv, in_sem.at[1])
    len_in = pltpu.make_async_copy(len_hbm, lens, in_sem.at[2])
    first_column = pl.multiple_of((tiles * part // parts) * LANES, LANES)
    w_in = pltpu.make_async_copy(
        w_hbm.at[:, pl.ds(first_column, span * LANES)], wbuf, in_sem.at[3]
    )
    k_in = [pltpu.make_async_copy(k_hbm.at[:, k], kbuf.at[k], k_sem.at[k]) for k in range(kv_count)]
    v_in = [pltpu.make_async_copy(v_hbm.at[:, k], vbuf.at[k], in_sem.at[4]) for k in range(kv_count)]
    for copy in [q_in, tab_in, len_in]:
        copy.start()
    for copy in [q_in, tab_in, len_in]:
        copy.wait()
    for copy in k_in + v_in:
        copy.start()
    pl.when(owns(me))(w_in.start)

    def to_seq(source, target, send, recv, to_owners=False):
        for j in reversed(range(1, n)):
            copy = pltpu.make_async_remote_copy(
                src_ref=source, dst_ref=target, send_sem=send, recv_sem=recv,
                device_id={"seq": seq_peer[j]}, device_id_type=MESH,
            )
            if to_owners:
                pl.when(owns(seq_peer[j]))(copy.start)
            else:
                copy.start()

    def wait_all(ref, sem):
        pltpu.make_async_copy(ref, ref, sem).wait()

    pl.semaphore_wait(barrier, n - 1 + jnp.where(owns(me), nz - 1, 0))
    to_seq(qall.at[own_rows], qall.at[own_rows], q_sem.at[0], q_sem.at[1])

    row = lax.broadcasted_iota(jnp.int32, (batch, LANES), 0)
    lane = lax.broadcasted_iota(jnp.int32, (batch, LANES), 1)
    length = jnp.zeros((batch, LANES), jnp.int32)
    for b in range(batch):
        length = jnp.where(row == b, lens[b], length)
    window_start = jnp.maximum(length - WINDOW, 0)
    first_block = lax.div(window_start, block_len)
    table = tabv[...]
    slot_lane = lane + me * slot_count
    rank = jnp.full((batch, LANES), -1, jnp.int32)
    for j in range(entries):
        rank = jnp.where(table[:, j : j + 1] == slot_lane, j, rank)
    base = (first_block + rank) * block_len
    low = jnp.where(rank >= 0, window_start - base, block_len)
    high = jnp.where(rank >= 0, length - base, 0)
    for p in range(slot_count):
        live = (lane >= low[:, p : p + 1]) & (lane < high[:, p : p + 1])
        bias[:, p * block_len : (p + 1) * block_len] = jnp.where(live, 0.0, lowest_score)

    for k in range(kv_count):
        k_in[k].wait()
        for p in range(slot_count):
            kflip[k, :, p * block_len : (p + 1) * block_len] = kbuf[k, p].T

    wait_all(vbuf, in_sem.at[4])
    wait_all(qall.at[pl.ds(0, (n - 1) * own_batch)], q_sem.at[1])
    for b in range(batch):
        qf[b * head_count : (b + 1) * head_count, :] = qall[b].astype(F32)

    chunk = 4 if slot_count % 4 == 0 else 1
    width = chunk * block_len
    chunks = slot_count // chunk

    def lane_tiles(x, op):
        out = x[:, :LANES]
        for c in range(1, x.shape[1] // LANES):
            out = op(out, x[:, c * LANES : (c + 1) * LANES])
        return out

    largest, totals = [], []

    def score(k):
        grouped = jnp.concatenate(
            [qf[pl.ds(k * group + g, batch, stride=head_count), :] for g in range(group)], axis=0
        ).astype(BF16)
        top = jnp.full((rows, LANES), lowest_largest, F32)
        for c in range(chunks):
            piece = slice(c * width, (c + 1) * width)
            s = jnp.dot(grouped, kflip[k, :, piece], preferred_element_type=F32)
            s = s * score_scale + jnp.concatenate([bias[:, piece]] * group, axis=0)
            scores[k, :, piece] = s
            top = jnp.maximum(top, lane_tiles(s, jnp.maximum))
        largest.append(jnp.max(top, axis=1, keepdims=True))

    def soften(k):
        total = jnp.zeros((rows, LANES), F32)
        for c in range(chunks):
            piece = slice(c * width, (c + 1) * width)
            weight = jnp.exp(scores[k, :, piece] - largest[k])
            total = total + lane_tiles(weight, jnp.add)
            probs[k, :, piece] = weight.astype(BF16)
        totals.append(jnp.sum(total, axis=1, keepdims=True))

    def share_totals():
        packed = jnp.ones((batch, LANES), F32)
        for k in range(kv_count):
            for g in range(group):
                h = k * group + g
                own = slice(g * batch, (g + 1) * batch)
                packed = jnp.where(lane == h, largest[k][own], packed)
                packed = jnp.where(lane == head_count + h, totals[k][own], packed)
        mlbuf[me] = packed
        to_seq(mlbuf.at[me], mlbuf.at[me], ml_sem.at[0], ml_sem.at[1], to_owners=True)

    def share_sums(k):
        values = vbuf[k].reshape(total_columns, head_width)
        obuf[k, me] = jnp.dot(probs[k], values, preferred_element_type=F32).astype(BF16)
        to_seq(obuf.at[k, me], obuf.at[k, me], o_send.at[0], o_recv.at[k], to_owners=True)

    for k in range(kv_count):
        score(k)
    for k in range(kv_count):
        soften(k)
    share_totals()
    for k in range(kv_count):
        share_sums(k)

    others = pl.ds(0, n - 1)

    @pl.when(owns(me))
    def _():
        wait_all(mlbuf.at[others], ml_sem.at[1])
        whole_largest = mlbuf[0]
        for i in range(1, n):
            whole_largest = jnp.maximum(whole_largest, mlbuf[i])
        whole_total = jnp.zeros((batch, LANES), F32)
        factors = []
        for i in range(n):
            factors.append(jnp.exp(mlbuf[i] - whole_largest))
            whole_total = whole_total + factors[i] * pltpu.roll(mlbuf[i], LANES - head_count, 1)
        inverse = 1.0 / whole_total
        for i in range(n):
            factor = factors[i] * inverse
            for h in range(head_count):
                wts[i, h] = jnp.broadcast_to(factor[:, h : h + 1], (batch, head_width))

        w_in.wait()
        partial_sum = jnp.zeros((batch, span * LANES), F32)
        depth = group * head_width
        for k in range(kv_count):
            wait_all(obuf.at[k, others], o_recv.at[k])
            sums = [jnp.zeros((batch, head_width), F32) for _ in range(group)]
            for i in range(n):
                arrived = obuf[k, i].astype(F32)
                for g in range(group):
                    own = slice(g * batch, (g + 1) * batch)
                    sums[g] = sums[g] + wts[i, k * group + g] * arrived[own]
            attention = jnp.concatenate(sums, axis=1).astype(BF16)
            partial_sum = partial_sum + jnp.dot(
                attention, wbuf[k * depth : (k + 1) * depth, :], preferred_element_type=F32
            )

        zbuf[mz] = partial_sum.astype(BF16)
        for j in reversed(range(1, nz)):
            pltpu.make_async_remote_copy(
                src_ref=zbuf.at[mz], dst_ref=zbuf.at[mz], send_sem=z_sem.at[0], recv_sem=z_sem.at[1],
                device_id={"head": head_peer[j]}, device_id_type=MESH,
            ).start()
        wait_all(zbuf.at[pl.ds(0, nz - 1)], z_sem.at[1])
        finished = zbuf[0].astype(F32)
        for z in range(1, nz):
            finished = finished + zbuf[z].astype(F32)
        fbuf[part] = finished.astype(BF16)
        to_seq(fbuf.at[part], fbuf.at[part], f_sem.at[0], f_sem.at[1])
        if parts > 1:
            wait_all(fbuf.at[pl.ds(0, parts - 1)], f_sem.at[1])

    if cores > 1:

        @pl.when(jnp.logical_not(owns(me)))
        def _():
            wait_all(fbuf.at[pl.ds(0, parts)], f_sem.at[1])

    for c in range(parts):
        if ends[c] > starts[c]:
            filled = (ends[c] - starts[c]) * LANES
            out_ref[:, starts[c] * LANES : ends[c] * LANES] = fbuf[c, :, :filled]
    wait_all(qall.at[pl.ds(0, (n - 1) * own_batch)], q_sem.at[0])

    @pl.when(owns(me))
    def _():
        if parts > 1:
            wait_all(mlbuf.at[pl.ds(0, parts - 1)], ml_sem.at[0])
            wait_all(obuf.at[:, pl.ds(0, parts - 1)], o_send.at[0])
        wait_all(zbuf.at[pl.ds(0, nz - 1)], z_sem.at[0])
        wait_all(fbuf.at[others], f_sem.at[0])

    if cores > 1:

        @pl.when(jnp.logical_not(owns(me)))
        def _():
            wait_all(mlbuf.at[pl.ds(0, parts)], ml_sem.at[0])
            wait_all(obuf.at[:, pl.ds(0, parts)], o_send.at[0])


def local(n, nz, queries, key_pool, value_pool, lengths, block_table, out_weight):
    slot_count, kv_count, block_len, head_width = key_pool.shape
    batch, entries = block_table.shape
    head_count = queries.shape[1]
    rows = head_count // kv_count * batch
    columns = slot_count * block_len
    depth, out_width = out_weight.shape
    _, _, _, span = column_tiles(out_width, n // cores_of(n))
    dma = pltpu.SemaphoreType.DMA
    hbm = pl.BlockSpec(memory_space=pl.ANY)
    return pl.pallas_call(
        functools.partial(kernel, n, nz),
        out_shape=pltpu.VMEM((batch, out_width), BF16),
        in_specs=[hbm] * 6,
        out_specs=pl.BlockSpec(memory_space=pltpu.VMEM),
        scratch_shapes=[
            pltpu.VMEM((kv_count, slot_count, block_len, head_width), BF16),
            pltpu.VMEM((kv_count, slot_count, block_len, head_width), BF16),
            pltpu.VMEM((depth, span * LANES), BF16),
            pltpu.VMEM((kv_count, head_width, columns), BF16),
            pltpu.VMEM((batch, head_count, head_width), BF16),
            pltpu.VMEM((batch * head_count, head_width), F32),
            pltpu.VMEM((batch, entries), jnp.int32),
            pltpu.SMEM((batch,), jnp.int32),
            pltpu.VMEM((batch, columns), F32),
            pltpu.VMEM((kv_count, rows, columns), F32),
            pltpu.VMEM((kv_count, rows, columns), BF16),
            pltpu.VMEM((n, batch, LANES), F32),
            pltpu.VMEM((kv_count, n, rows, head_width), BF16),
            pltpu.VMEM((n, head_count, batch, head_width), F32),
            pltpu.VMEM((nz, batch, span * LANES), BF16),
            pltpu.VMEM((n, batch, span * LANES), BF16),
            dma((5,)), dma((kv_count,)), dma((2,)), dma((2,)),
            dma((1,)), dma((kv_count,)), dma((2,)), dma((2,)),
        ],
        compiler_params=pltpu.CompilerParams(
            collective_id=0, has_side_effects=True, vmem_limit_bytes=56 * 1024 * 1024
        ),
    )(queries, key_pool, value_pool, lengths, block_table, out_weight)


def solution(mesh):
    return jax.shard_map(
        functools.partial(local, mesh.shape["seq"], mesh.shape["head"]),
        mesh=mesh,
        in_specs=(
            P("seq", "head", None),
            P("seq", "head", None, None),
            P("seq", "head", None, None),
            P(),
            P(),
            P("head", None),
        ),
        out_specs=P(),
        check_vma=False,
    )
```

```python
import functools

import jax
import jax.numpy as jnp
from jax import lax
from jax.experimental import pallas as pl
from jax.experimental.pallas import tpu as pltpu
from jax.sharding import PartitionSpec as P

WINDOW = 4096

lowest_score = -1e30
lowest_largest = -1e29
score_scale = 1.0 / 12.0
LANES = 128
F32 = jnp.float32
BF16 = jnp.bfloat16
MESH = pl.DeviceIdType.MESH


def column_tiles(width, parts):
    tiles = width // LANES
    starts = [tiles * i // parts for i in range(parts)]
    ends = starts[1:] + [tiles]
    span = max(e - s for s, e in zip(starts, ends))
    return tiles, starts, ends, span


def cores_of(n):
    return 2 if n % 2 == 0 else 1


def peer_index(index, step, size):
    if size & (size - 1):
        return lax.rem(index + step, size)
    peer, bit = 0, 1
    while bit < size:
        own = lax.rem(lax.div(index, bit), 2)
        peer = peer + bit * ((1 - own) if step & bit else own)
        bit *= 2
    return peer


def kernel(
    n, nz,
    q_hbm, k_hbm, v_hbm, len_hbm, tab_hbm, w_hbm, out_ref,
    kbuf, vbuf, wbuf, kflip, qall, qf, tabv, lens, bias, scores, probs,
    mlbuf, obuf, wts, zbuf, fbuf,
    in_sem, k_sem, q_sem, ml_sem, o_send, o_recv, z_sem, f_sem,
):
    me = lax.axis_index("seq")
    mz = lax.axis_index("head")
    slot_count, kv_count, block_len, head_width = k_hbm.shape
    batch, entries = tab_hbm.shape
    own_batch, head_count = q_hbm.shape[0], q_hbm.shape[1]
    group = head_count // kv_count
    cores = cores_of(n)
    parts, part = n // cores, lax.div(me, cores)
    rows = group * batch
    tiles, starts, ends, span = column_tiles(w_hbm.shape[1], parts)

    def owns(index):
        return lax.rem(index, cores) == cores - 1

    total_columns = slot_count * block_len
    seq_peer = [peer_index(me, j, n) for j in range(n)]
    head_peer = [peer_index(mz, j, nz) for j in range(nz)]

    barrier = pltpu.get_barrier_semaphore()
    for j in reversed(range(1, n)):
        pl.semaphore_signal(barrier, inc=1, device_id={"seq": seq_peer[j]}, device_id_type=MESH)

    @pl.when(owns(me))
    def _():
        for j in reversed(range(1, nz)):
            pl.semaphore_signal(
                barrier, inc=1, device_id={"head": head_peer[j]}, device_id_type=MESH
            )

    own_rows = pl.ds(me * own_batch, own_batch)
    q_in = pltpu.make_async_copy(q_hbm, qall.at[own_rows], in_sem.at[0])
    tab_in = pltpu.make_async_copy(tab_hbm, tabv, in_sem.at[1])
    len_in = pltpu.make_async_copy(len_hbm, lens, in_sem.at[2])
    first_column = pl.multiple_of((tiles * part // parts) * LANES, LANES)
    w_in = pltpu.make_async_copy(
        w_hbm.at[:, pl.ds(first_column, span * LANES)], wbuf, in_sem.at[3]
    )
    k_in = [pltpu.make_async_copy(k_hbm.at[:, k], kbuf.at[k], k_sem.at[k]) for k in range(kv_count)]
    v_in = [pltpu.make_async_copy(v_hbm.at[:, k], vbuf.at[k], in_sem.at[4]) for k in range(kv_count)]
    for copy in [q_in, tab_in, len_in]:
        copy.start()
    q_in.wait()
    for copy in k_in:
        copy.start()

    def to_seq(source, target, send, recv, to_owners=False):
        def copy(index):
            return pltpu.make_async_remote_copy(
                src_ref=source, dst_ref=target, send_sem=send, recv_sem=recv,
                device_id={"seq": index}, device_id_type=MESH,
            )

        if not to_owners:
            for j in reversed(range(1, n)):
                copy(seq_peer[j]).start()
            return
        for j in reversed(range(1, parts)):
            copy(peer_index(part, j, parts) * cores + cores - 1).start()
        if cores > 1:
            pl.when(jnp.logical_not(owns(me)))(copy(part * cores + cores - 1).start)

    def wait_all(ref, sem):
        pltpu.make_async_copy(ref, ref, sem).wait()

    pl.semaphore_wait(barrier, n - 1 + jnp.where(owns(me), nz - 1, 0))
    to_seq(qall.at[own_rows], qall.at[own_rows], q_sem.at[0], q_sem.at[1])

    tab_in.wait()
    len_in.wait()
    row = lax.broadcasted_iota(jnp.int32, (batch, LANES), 0)
    lane = lax.broadcasted_iota(jnp.int32, (batch, LANES), 1)
    length = jnp.zeros((batch, LANES), jnp.int32)
    for b in range(batch):
        length = jnp.where(row == b, lens[b], length)
    window_start = jnp.maximum(length - WINDOW, 0)
    first_block = lax.div(window_start, block_len)
    table = tabv[...]
    slot_lane = lane + me * slot_count
    rank = jnp.full((batch, LANES), -1, jnp.int32)
    for j in range(entries):
        rank = jnp.where(table[:, j : j + 1] == slot_lane, j, rank)
    base = (first_block + rank) * block_len
    low = jnp.where(rank >= 0, window_start - base, block_len)
    high = jnp.where(rank >= 0, length - base, 0)
    for p in range(slot_count):
        live = (lane >= low[:, p : p + 1]) & (lane < high[:, p : p + 1])
        bias[:, p * block_len : (p + 1) * block_len] = jnp.where(live, 0.0, lowest_score)

    for k in range(kv_count):
        k_in[k].wait()
        v_in[k].start()
        for p in range(slot_count):
            kflip[k, :, p * block_len : (p + 1) * block_len] = kbuf[k, p].T

    pl.when(owns(me))(w_in.start)
    wait_all(qall.at[pl.ds(0, (n - 1) * own_batch)], q_sem.at[1])
    for b in range(batch):
        qf[b * head_count : (b + 1) * head_count, :] = qall[b].astype(F32)

    chunk = 4 if slot_count % 4 == 0 else 1
    width = chunk * block_len
    chunks = slot_count // chunk

    def lane_tiles(x, op):
        out = x[:, :LANES]
        for c in range(1, x.shape[1] // LANES):
            out = op(out, x[:, c * LANES : (c + 1) * LANES])
        return out

    largest, totals = [], []

    def score(k):
        grouped = jnp.concatenate(
            [qf[pl.ds(k * group + g, batch, stride=head_count), :] for g in range(group)], axis=0
        ).astype(BF16)
        top = jnp.full((rows, LANES), lowest_largest, F32)
        for c in range(chunks):
            piece = slice(c * width, (c + 1) * width)
            s = jnp.dot(grouped, kflip[k, :, piece], preferred_element_type=F32)
            s = s * score_scale + jnp.concatenate([bias[:, piece]] * group, axis=0)
            scores[k, :, piece] = s
            top = jnp.maximum(top, lane_tiles(s, jnp.maximum))
        largest.append(jnp.max(top, axis=1, keepdims=True))

    def soften(k):
        total = jnp.zeros((rows, LANES), F32)
        for c in range(chunks):
            piece = slice(c * width, (c + 1) * width)
            weight = jnp.exp(scores[k, :, piece] - largest[k])
            total = total + lane_tiles(weight, jnp.add)
            probs[k, :, piece] = weight.astype(BF16)
        totals.append(jnp.sum(total, axis=1, keepdims=True))

    def share_totals():
        packed = jnp.ones((batch, LANES), F32)
        for k in range(kv_count):
            for g in range(group):
                h = k * group + g
                own = slice(g * batch, (g + 1) * batch)
                packed = jnp.where(lane == h, largest[k][own], packed)
                packed = jnp.where(lane == head_count + h, totals[k][own], packed)
        mlbuf[me] = packed
        to_seq(mlbuf.at[me], mlbuf.at[me], ml_sem.at[0], ml_sem.at[1], to_owners=True)

    def share_sums(k):
        values = vbuf[k].reshape(total_columns, head_width)
        obuf[k, me] = jnp.dot(probs[k], values, preferred_element_type=F32).astype(BF16)
        to_seq(obuf.at[k, me], obuf.at[k, me], o_send.at[0], o_recv.at[k], to_owners=True)

    for k in range(kv_count):
        score(k)
    for k in range(kv_count):
        soften(k)
    share_totals()
    wait_all(vbuf, in_sem.at[4])
    for k in range(kv_count):
        share_sums(k)

    others = pl.ds(0, n - 1)

    @pl.when(owns(me))
    def _():
        wait_all(mlbuf.at[others], ml_sem.at[1])
        whole_largest = mlbuf[0]
        for i in range(1, n):
            whole_largest = jnp.maximum(whole_largest, mlbuf[i])
        whole_total = jnp.zeros((batch, LANES), F32)
        factors = []
        for i in range(n):
            factors.append(jnp.exp(mlbuf[i] - whole_largest))
            whole_total = whole_total + factors[i] * pltpu.roll(mlbuf[i], LANES - head_count, 1)
        inverse = 1.0 / whole_total
        for i in range(n):
            factor = factors[i] * inverse
            for h in range(head_count):
                wts[i, h] = jnp.broadcast_to(factor[:, h : h + 1], (batch, head_width))

        w_in.wait()
        partial_sum = jnp.zeros((batch, span * LANES), F32)
        depth = group * head_width
        for k in range(kv_count):
            wait_all(obuf.at[k, others], o_recv.at[k])
            sums = [jnp.zeros((batch, head_width), F32) for _ in range(group)]
            for i in range(n):
                arrived = obuf[k, i].astype(F32)
                for g in range(group):
                    own = slice(g * batch, (g + 1) * batch)
                    sums[g] = sums[g] + wts[i, k * group + g] * arrived[own]
            attention = jnp.concatenate(sums, axis=1).astype(BF16)
            partial_sum = partial_sum + jnp.dot(
                attention, wbuf[k * depth : (k + 1) * depth, :], preferred_element_type=F32
            )

        zbuf[mz] = partial_sum.astype(BF16)
        for j in reversed(range(1, nz)):
            pltpu.make_async_remote_copy(
                src_ref=zbuf.at[mz], dst_ref=zbuf.at[mz], send_sem=z_sem.at[0], recv_sem=z_sem.at[1],
                device_id={"head": head_peer[j]}, device_id_type=MESH,
            ).start()
        wait_all(zbuf.at[pl.ds(0, nz - 1)], z_sem.at[1])
        finished = zbuf[0].astype(F32)
        for z in range(1, nz):
            finished = finished + zbuf[z].astype(F32)
        fbuf[part] = finished.astype(BF16)
        to_seq(fbuf.at[part], fbuf.at[part], f_sem.at[0], f_sem.at[1])
        if parts > 1:
            wait_all(fbuf.at[pl.ds(0, parts - 1)], f_sem.at[1])

    if cores > 1:

        @pl.when(jnp.logical_not(owns(me)))
        def _():
            wait_all(fbuf.at[pl.ds(0, parts)], f_sem.at[1])

    for c in range(parts):
        if ends[c] > starts[c]:
            filled = (ends[c] - starts[c]) * LANES
            out_ref[:, starts[c] * LANES : ends[c] * LANES] = fbuf[c, :, :filled]
    wait_all(qall.at[pl.ds(0, (n - 1) * own_batch)], q_sem.at[0])

    @pl.when(owns(me))
    def _():
        if parts > 1:
            wait_all(mlbuf.at[pl.ds(0, parts - 1)], ml_sem.at[0])
            wait_all(obuf.at[:, pl.ds(0, parts - 1)], o_send.at[0])
        wait_all(zbuf.at[pl.ds(0, nz - 1)], z_sem.at[0])
        wait_all(fbuf.at[others], f_sem.at[0])

    if cores > 1:

        @pl.when(jnp.logical_not(owns(me)))
        def _():
            wait_all(mlbuf.at[pl.ds(0, parts)], ml_sem.at[0])
            wait_all(obuf.at[:, pl.ds(0, parts)], o_send.at[0])


def local(n, nz, queries, key_pool, value_pool, lengths, block_table, out_weight):
    slot_count, kv_count, block_len, head_width = key_pool.shape
    batch, entries = block_table.shape
    head_count = queries.shape[1]
    rows = head_count // kv_count * batch
    columns = slot_count * block_len
    depth, out_width = out_weight.shape
    _, _, _, span = column_tiles(out_width, n // cores_of(n))
    dma = pltpu.SemaphoreType.DMA
    hbm = pl.BlockSpec(memory_space=pl.ANY)
    return pl.pallas_call(
        functools.partial(kernel, n, nz),
        out_shape=pltpu.VMEM((batch, out_width), BF16),
        in_specs=[hbm] * 6,
        out_specs=pl.BlockSpec(memory_space=pltpu.VMEM),
        scratch_shapes=[
            pltpu.VMEM((kv_count, slot_count, block_len, head_width), BF16),
            pltpu.VMEM((kv_count, slot_count, block_len, head_width), BF16),
            pltpu.VMEM((depth, span * LANES), BF16),
            pltpu.VMEM((kv_count, head_width, columns), BF16),
            pltpu.VMEM((batch, head_count, head_width), BF16),
            pltpu.VMEM((batch * head_count, head_width), F32),
            pltpu.VMEM((batch, entries), jnp.int32),
            pltpu.SMEM((batch,), jnp.int32),
            pltpu.VMEM((batch, columns), F32),
            pltpu.VMEM((kv_count, rows, columns), F32),
            pltpu.VMEM((kv_count, rows, columns), BF16),
            pltpu.VMEM((n, batch, LANES), F32),
            pltpu.VMEM((kv_count, n, rows, head_width), BF16),
            pltpu.VMEM((n, head_count, batch, head_width), F32),
            pltpu.VMEM((nz, batch, span * LANES), BF16),
            pltpu.VMEM((n, batch, span * LANES), BF16),
            dma((5,)), dma((kv_count,)), dma((2,)), dma((2,)),
            dma((1,)), dma((kv_count,)), dma((2,)), dma((2,)),
        ],
        compiler_params=pltpu.CompilerParams(
            collective_id=0, has_side_effects=True, vmem_limit_bytes=56 * 1024 * 1024
        ),
    )(queries, key_pool, value_pool, lengths, block_table, out_weight)


def solution(mesh):
    return jax.shard_map(
        functools.partial(local, mesh.shape["seq"], mesh.shape["head"]),
        mesh=mesh,
        in_specs=(
            P("seq", "head", None),
            P("seq", "head", None, None),
            P("seq", "head", None, None),
            P(),
            P(),
            P("head", None),
        ),
        out_specs=P(),
        check_vma=False,
    )
```

```python
import functools

import jax
import jax.numpy as jnp
from jax import lax
from jax.experimental import pallas as pl
from jax.experimental.pallas import tpu as pltpu
from jax.sharding import PartitionSpec as P

WINDOW = 4096

lowest_score = -1e30
lowest_largest = -1e29
score_scale = 1.0 / 12.0
LANES = 128
F32 = jnp.float32
BF16 = jnp.bfloat16
MESH = pl.DeviceIdType.MESH


def column_tiles(width, parts):
    tiles = width // LANES
    starts = [tiles * i // parts for i in range(parts)]
    ends = starts[1:] + [tiles]
    span = max(e - s for s, e in zip(starts, ends))
    return tiles, starts, ends, span


def cores_of(n):
    return 2 if n % 2 == 0 else 1


def peer_index(index, step, size):
    if size & (size - 1):
        return lax.rem(index + step, size)
    peer, bit = 0, 1
    while bit < size:
        own = lax.rem(lax.div(index, bit), 2)
        peer = peer + bit * ((1 - own) if step & bit else own)
        bit *= 2
    return peer


def kernel(
    n, nz,
    q_hbm, k_hbm, v_hbm, len_hbm, tab_hbm, w_hbm, out_ref,
    kbuf, vbuf, wbuf, kflip, qall, qf, tabv, lens, bias, scores, probs,
    mlbuf, obuf, wts, zbuf, fbuf,
    in_sem, k_sem, v_sem, q_sem, ml_sem, o_send, o_recv, z_sem, f_sem,
):
    me = lax.axis_index("seq")
    mz = lax.axis_index("head")
    slot_count, kv_count, block_len, head_width = k_hbm.shape
    batch, entries = tab_hbm.shape
    own_batch, head_count = q_hbm.shape[0], q_hbm.shape[1]
    group = head_count // kv_count
    cores = cores_of(n)
    parts, part = n // cores, lax.div(me, cores)
    rows = group * batch
    tiles, starts, ends, span = column_tiles(w_hbm.shape[1], parts)

    def owns(index):
        return lax.rem(index, cores) == cores - 1

    total_columns = slot_count * block_len
    seq_peer = [peer_index(me, j, n) for j in range(n)]
    head_peer = [peer_index(mz, j, nz) for j in range(nz)]

    barrier = pltpu.get_barrier_semaphore()
    for j in reversed(range(1, n)):
        pl.semaphore_signal(barrier, inc=1, device_id={"seq": seq_peer[j]}, device_id_type=MESH)

    @pl.when(owns(me))
    def _():
        for j in reversed(range(1, nz)):
            pl.semaphore_signal(
                barrier, inc=1, device_id={"head": head_peer[j]}, device_id_type=MESH
            )

    own_rows = pl.ds(me * own_batch, own_batch)
    q_in = pltpu.make_async_copy(q_hbm, qall.at[own_rows], in_sem.at[0])
    tab_in = pltpu.make_async_copy(tab_hbm, tabv, in_sem.at[1])
    len_in = pltpu.make_async_copy(len_hbm, lens, in_sem.at[2])
    first_column = pl.multiple_of((tiles * part // parts) * LANES, LANES)
    w_in = pltpu.make_async_copy(
        w_hbm.at[:, pl.ds(first_column, span * LANES)], wbuf, in_sem.at[3]
    )
    k_in = [pltpu.make_async_copy(k_hbm.at[:, k], kbuf.at[k], k_sem.at[k]) for k in range(kv_count)]
    v_in = [pltpu.make_async_copy(v_hbm.at[:, k], vbuf.at[k], v_sem.at[k]) for k in range(kv_count)]
    for copy in [q_in, tab_in, len_in]:
        copy.start()
    q_in.wait()
    for copy in k_in:
        copy.start()

    def to_seq(source, target, send, recv, to_owners=False):
        def copy(index):
            return pltpu.make_async_remote_copy(
                src_ref=source, dst_ref=target, send_sem=send, recv_sem=recv,
                device_id={"seq": index}, device_id_type=MESH,
            )

        if not to_owners:
            for j in reversed(range(1, n)):
                copy(seq_peer[j]).start()
            return
        for j in reversed(range(1, parts)):
            copy(peer_index(part, j, parts) * cores + cores - 1).start()
        if cores > 1:
            pl.when(jnp.logical_not(owns(me)))(copy(part * cores + cores - 1).start)

    def wait_all(ref, sem):
        pltpu.make_async_copy(ref, ref, sem).wait()

    pl.semaphore_wait(barrier, n - 1 + jnp.where(owns(me), nz - 1, 0))
    to_seq(qall.at[own_rows], qall.at[own_rows], q_sem.at[0], q_sem.at[1])

    tab_in.wait()
    len_in.wait()
    row = lax.broadcasted_iota(jnp.int32, (batch, LANES), 0)
    lane = lax.broadcasted_iota(jnp.int32, (batch, LANES), 1)
    length = jnp.zeros((batch, LANES), jnp.int32)
    for b in range(batch):
        length = jnp.where(row == b, lens[b], length)
    window_start = jnp.maximum(length - WINDOW, 0)
    first_block = lax.div(window_start, block_len)
    table = tabv[...]
    slot_lane = lane + me * slot_count
    rank = jnp.full((batch, LANES), -1, jnp.int32)
    for j in range(entries):
        rank = jnp.where(table[:, j : j + 1] == slot_lane, j, rank)
    base = (first_block + rank) * block_len
    low = jnp.where(rank >= 0, window_start - base, block_len)
    high = jnp.where(rank >= 0, length - base, 0)
    for p in range(slot_count):
        live = (lane >= low[:, p : p + 1]) & (lane < high[:, p : p + 1])
        bias[:, p * block_len : (p + 1) * block_len] = jnp.where(live, 0.0, lowest_score)

    for k in range(kv_count):
        k_in[k].wait()
        v_in[k].start()
        for p in range(slot_count):
            kflip[k, :, p * block_len : (p + 1) * block_len] = kbuf[k, p].T

    pl.when(owns(me))(w_in.start)
    wait_all(qall.at[pl.ds(0, (n - 1) * own_batch)], q_sem.at[1])
    for b in range(batch):
        qf[b * head_count : (b + 1) * head_count, :] = qall[b].astype(F32)

    chunk = 4 if slot_count % 4 == 0 else 1
    width = chunk * block_len
    chunks = slot_count // chunk

    def lane_tiles(x, op):
        out = x[:, :LANES]
        for c in range(1, x.shape[1] // LANES):
            out = op(out, x[:, c * LANES : (c + 1) * LANES])
        return out

    largest, totals = [], []

    def score(k):
        grouped = jnp.concatenate(
            [qf[pl.ds(k * group + g, batch, stride=head_count), :] for g in range(group)], axis=0
        ).astype(BF16)
        top = jnp.full((rows, LANES), lowest_largest, F32)
        for c in range(chunks):
            piece = slice(c * width, (c + 1) * width)
            s = jnp.dot(grouped, kflip[k, :, piece], preferred_element_type=F32)
            s = s * score_scale + jnp.concatenate([bias[:, piece]] * group, axis=0)
            scores[k, :, piece] = s
            top = jnp.maximum(top, lane_tiles(s, jnp.maximum))
        largest.append(jnp.max(top, axis=1, keepdims=True))

    def soften(k):
        total = jnp.zeros((rows, LANES), F32)
        for c in range(chunks):
            piece = slice(c * width, (c + 1) * width)
            weight = jnp.exp(scores[k, :, piece] - largest[k])
            total = total + lane_tiles(weight, jnp.add)
            probs[k, :, piece] = weight.astype(BF16)
        totals.append(jnp.sum(total, axis=1, keepdims=True))

    def share_totals():
        packed = jnp.ones((batch, LANES), F32)
        for k in range(kv_count):
            for g in range(group):
                h = k * group + g
                own = slice(g * batch, (g + 1) * batch)
                packed = jnp.where(lane == h, largest[k][own], packed)
                packed = jnp.where(lane == head_count + h, totals[k][own], packed)
        mlbuf[me] = packed
        to_seq(mlbuf.at[me], mlbuf.at[me], ml_sem.at[0], ml_sem.at[1], to_owners=True)

    def share_sums(k):
        values = vbuf[k].reshape(total_columns, head_width)
        obuf[k, me] = jnp.dot(probs[k], values, preferred_element_type=F32).astype(BF16)
        to_seq(obuf.at[k, me], obuf.at[k, me], o_send.at[0], o_recv.at[k], to_owners=True)

    for k in range(kv_count):
        score(k)
    for k in range(kv_count):
        soften(k)
    share_totals()
    for k in range(kv_count):
        v_in[k].wait()
        share_sums(k)

    others = pl.ds(0, n - 1)

    @pl.when(owns(me))
    def _():
        wait_all(mlbuf.at[others], ml_sem.at[1])
        whole_largest = mlbuf[0]
        for i in range(1, n):
            whole_largest = jnp.maximum(whole_largest, mlbuf[i])
        whole_total = jnp.zeros((batch, LANES), F32)
        factors = []
        for i in range(n):
            factors.append(jnp.exp(mlbuf[i] - whole_largest))
            whole_total = whole_total + factors[i] * pltpu.roll(mlbuf[i], LANES - head_count, 1)
        inverse = 1.0 / whole_total
        for i in range(n):
            factor = factors[i] * inverse
            for h in range(head_count):
                wts[i, h] = jnp.broadcast_to(factor[:, h : h + 1], (batch, head_width))

        w_in.wait()
        partial_sum = jnp.zeros((batch, span * LANES), F32)
        depth = group * head_width
        for k in range(kv_count):
            wait_all(obuf.at[k, others], o_recv.at[k])
            sums = [jnp.zeros((batch, head_width), F32) for _ in range(group)]
            for i in range(n):
                arrived = obuf[k, i].astype(F32)
                for g in range(group):
                    own = slice(g * batch, (g + 1) * batch)
                    sums[g] = sums[g] + wts[i, k * group + g] * arrived[own]
            attention = jnp.concatenate(sums, axis=1).astype(BF16)
            partial_sum = partial_sum + jnp.dot(
                attention, wbuf[k * depth : (k + 1) * depth, :], preferred_element_type=F32
            )

        zbuf[mz] = partial_sum.astype(BF16)
        for j in reversed(range(1, nz)):
            pltpu.make_async_remote_copy(
                src_ref=zbuf.at[mz], dst_ref=zbuf.at[mz], send_sem=z_sem.at[0], recv_sem=z_sem.at[1],
                device_id={"head": head_peer[j]}, device_id_type=MESH,
            ).start()
        wait_all(zbuf.at[pl.ds(0, nz - 1)], z_sem.at[1])
        finished = zbuf[0].astype(F32)
        for z in range(1, nz):
            finished = finished + zbuf[z].astype(F32)
        fbuf[part] = finished.astype(BF16)
        to_seq(fbuf.at[part], fbuf.at[part], f_sem.at[0], f_sem.at[1])
        if parts > 1:
            wait_all(fbuf.at[pl.ds(0, parts - 1)], f_sem.at[1])

    if cores > 1:

        @pl.when(jnp.logical_not(owns(me)))
        def _():
            wait_all(fbuf.at[pl.ds(0, parts)], f_sem.at[1])

    for c in range(parts):
        if ends[c] > starts[c]:
            filled = (ends[c] - starts[c]) * LANES
            out_ref[:, starts[c] * LANES : ends[c] * LANES] = fbuf[c, :, :filled]
    wait_all(qall.at[pl.ds(0, (n - 1) * own_batch)], q_sem.at[0])

    @pl.when(owns(me))
    def _():
        if parts > 1:
            wait_all(mlbuf.at[pl.ds(0, parts - 1)], ml_sem.at[0])
            wait_all(obuf.at[:, pl.ds(0, parts - 1)], o_send.at[0])
        wait_all(zbuf.at[pl.ds(0, nz - 1)], z_sem.at[0])
        wait_all(fbuf.at[others], f_sem.at[0])

    if cores > 1:

        @pl.when(jnp.logical_not(owns(me)))
        def _():
            wait_all(mlbuf.at[pl.ds(0, parts)], ml_sem.at[0])
            wait_all(obuf.at[:, pl.ds(0, parts)], o_send.at[0])


def local(n, nz, queries, key_pool, value_pool, lengths, block_table, out_weight):
    slot_count, kv_count, block_len, head_width = key_pool.shape
    batch, entries = block_table.shape
    head_count = queries.shape[1]
    rows = head_count // kv_count * batch
    columns = slot_count * block_len
    depth, out_width = out_weight.shape
    _, _, _, span = column_tiles(out_width, n // cores_of(n))
    dma = pltpu.SemaphoreType.DMA
    hbm = pl.BlockSpec(memory_space=pl.ANY)
    return pl.pallas_call(
        functools.partial(kernel, n, nz),
        out_shape=pltpu.VMEM((batch, out_width), BF16),
        in_specs=[hbm] * 6,
        out_specs=pl.BlockSpec(memory_space=pltpu.VMEM),
        scratch_shapes=[
            pltpu.VMEM((kv_count, slot_count, block_len, head_width), BF16),
            pltpu.VMEM((kv_count, slot_count, block_len, head_width), BF16),
            pltpu.VMEM((depth, span * LANES), BF16),
            pltpu.VMEM((kv_count, head_width, columns), BF16),
            pltpu.VMEM((batch, head_count, head_width), BF16),
            pltpu.VMEM((batch * head_count, head_width), F32),
            pltpu.VMEM((batch, entries), jnp.int32),
            pltpu.SMEM((batch,), jnp.int32),
            pltpu.VMEM((batch, columns), F32),
            pltpu.VMEM((kv_count, rows, columns), F32),
            pltpu.VMEM((kv_count, rows, columns), BF16),
            pltpu.VMEM((n, batch, LANES), F32),
            pltpu.VMEM((kv_count, n, rows, head_width), BF16),
            pltpu.VMEM((n, head_count, batch, head_width), F32),
            pltpu.VMEM((nz, batch, span * LANES), BF16),
            pltpu.VMEM((n, batch, span * LANES), BF16),
            dma((4,)), dma((kv_count,)), dma((kv_count,)), dma((2,)), dma((2,)),
            dma((1,)), dma((kv_count,)), dma((2,)), dma((2,)),
        ],
        compiler_params=pltpu.CompilerParams(
            collective_id=0, has_side_effects=True, vmem_limit_bytes=56 * 1024 * 1024
        ),
    )(queries, key_pool, value_pool, lengths, block_table, out_weight)


def solution(mesh):
    return jax.shard_map(
        functools.partial(local, mesh.shape["seq"], mesh.shape["head"]),
        mesh=mesh,
        in_specs=(
            P("seq", "head", None),
            P("seq", "head", None, None),
            P("seq", "head", None, None),
            P(),
            P(),
            P("head", None),
        ),
        out_specs=P(),
        check_vma=False,
    )
```
